32 devices in a mesh: dp: 4 (over z), ep: 8 (over y, x, core).
Axes of the slice: x: 2, y: 2, z: 4, core: 2. Of those that a mesh axis runs over, the one named last changes fastest.
Arguments:
- hidden: bfloat16 [8192, 1280], P(('dp', 'ep')), parts along dimension 0
- norm_gain: float32 [1280], replicated
- router_w: bfloat16 [1280, 64], replicated
- topk_idx: int32 [8192, 6], P(('dp', 'ep')), parts along dimension 0
- w_gate: bfloat16 [64, 1280, 896], P('ep')
- w_up: bfloat16 [64, 1280, 896], P('ep')
- w_down: bfloat16 [64, 896, 1280], P('ep')
- shared_gate: bfloat16 [1280, 1792], replicated
- shared_up: bfloat16 [1280, 1792], replicated
- shared_down: bfloat16 [1792, 1280], replicated
Outputs:
- output: bfloat16 [8192, 1280], P(('dp', 'ep')), parts along dimension 0
There are 4 independent parts. The reference program is written for one: setup_inputs(seed, part) draws one part's arguments, and reference() takes and returns one part's arrays. A program takes and returns all parts, laid end to end along the dimension named above; an argument that names none is the same for every part.
All inputs are finite; a program needn't handle non-finite values.
Results may differ from the reference program's by a relative error of at most 0.001.
Values are sent between devices in bfloat16 or wider.
A program may use at most 1 GiB of HBM per device.

```python
import jax
import jax.numpy as jnp
from jax import lax

HIDDEN = 1280
EXPERTS = 64
TOP_K = 6
EXPERT_FF = 896
SHARED_FF = 1792
GROUP_SIZE = 8
TOKENS = 256
ROW_BLOCK = 128
NORM_EPS = 1e-6

NUM_TOKENS = GROUP_SIZE * TOKENS
ROUTE_ROWS = NUM_TOKENS * TOP_K
NUM_BLOCKS = (ROUTE_ROWS + EXPERTS * (ROW_BLOCK - 1) + ROW_BLOCK - 1) // ROW_BLOCK


def draw_routing(route_key):
    mean_rows = TOKENS * TOP_K // EXPERTS
    half_rows = mean_rows // 2

    def one_device(dev_key):
        key_pair, key_shift, key_layout, key_tokens = jax.random.split(dev_key, 4)
        pair_perm = jax.random.permutation(key_pair, EXPERTS)
        shift_rows = jax.random.randint(key_shift, (EXPERTS // 2,), -half_rows, half_rows + 1)
        shift_rows = shift_rows.at[0].set(half_rows)
        pair_counts = jnp.stack([mean_rows + shift_rows, mean_rows - shift_rows], axis=1).reshape(EXPERTS)
        counts = jnp.zeros((EXPERTS,), jnp.int32).at[pair_perm].set(pair_counts)
        layout_order = jax.random.permutation(key_layout, EXPERTS)
        bounds = jnp.cumsum(counts[layout_order])
        positions = jnp.arange(TOKENS * TOP_K)
        range_index = jnp.sum(positions[:, None] >= bounds[None, :], axis=1)
        expert_grid = layout_order[range_index].reshape(TOP_K, TOKENS)
        token_perm = jax.random.permutation(key_tokens, TOKENS)
        return jnp.zeros((TOKENS, TOP_K), jnp.int32).at[token_perm].set(expert_grid.T)

    dev_keys = jax.random.split(route_key, GROUP_SIZE)
    return jax.vmap(one_device)(dev_keys).reshape(NUM_TOKENS, TOP_K).astype(jnp.int32)


def setup_inputs(seed: int = 0, part: int = 0) -> dict:
    base_key = jax.random.key(seed)
    part_key = jax.random.fold_in(base_key, part)
    key_hidden, key_route = jax.random.split(part_key, 2)
    weight_keys = jax.random.split(base_key, 8)
    in_scale = HIDDEN ** -0.5
    down_scale = (EXPERTS / TOP_K) * EXPERT_FF ** -0.5
    hidden = 0.5 * jax.random.normal(key_hidden, (NUM_TOKENS, HIDDEN), jnp.float32)
    norm_gain = jax.random.uniform(weight_keys[0], (HIDDEN,), jnp.float32, 0.5, 1.5)
    router_w = in_scale * jax.random.normal(weight_keys[1], (HIDDEN, EXPERTS), jnp.float32)
    w_gate = in_scale * jax.random.normal(weight_keys[2], (EXPERTS, HIDDEN, EXPERT_FF), jnp.float32)
    w_up = in_scale * jax.random.normal(weight_keys[3], (EXPERTS, HIDDEN, EXPERT_FF), jnp.float32)
    w_down = down_scale * jax.random.normal(weight_keys[4], (EXPERTS, EXPERT_FF, HIDDEN), jnp.float32)
    shared_gate = in_scale * jax.random.normal(weight_keys[5], (HIDDEN, SHARED_FF), jnp.float32)
    shared_up = in_scale * jax.random.normal(weight_keys[6], (HIDDEN, SHARED_FF), jnp.float32)
    shared_down = 0.5 * SHARED_FF ** -0.5 * jax.random.normal(weight_keys[7], (SHARED_FF, HIDDEN), jnp.float32)
    return {
        'hidden': hidden.astype(jnp.bfloat16),
        'norm_gain': norm_gain,
        'router_w': router_w.astype(jnp.bfloat16),
        'topk_idx': draw_routing(key_route),
        'w_gate': w_gate.astype(jnp.bfloat16),
        'w_up': w_up.astype(jnp.bfloat16),
        'w_down': w_down.astype(jnp.bfloat16),
        'shared_gate': shared_gate.astype(jnp.bfloat16),
        'shared_up': shared_up.astype(jnp.bfloat16),
        'shared_down': shared_down.astype(jnp.bfloat16),
    }


def rms_norm(hidden, norm_gain):
    hidden_f32 = hidden.astype(jnp.float32)
    inv_rms = lax.rsqrt(jnp.mean(hidden_f32 * hidden_f32, axis=-1, keepdims=True) + NORM_EPS)
    return (hidden_f32 * inv_rms * norm_gain).astype(jnp.bfloat16)


def swiglu_rows(rows_in, gate_w, up_w, down_w):
    gate_out = jnp.dot(rows_in, gate_w, preferred_element_type=jnp.float32)
    up_out = jnp.dot(rows_in, up_w, preferred_element_type=jnp.float32)
    activated = (jax.nn.silu(gate_out) * up_out).astype(jnp.bfloat16)
    return jnp.dot(activated, down_w, preferred_element_type=jnp.float32)


def reference(hidden, norm_gain, router_w, topk_idx, w_gate, w_up, w_down, shared_gate, shared_up, shared_down):
    normed = rms_norm(hidden, norm_gain)
    logits = jnp.dot(normed, router_w, preferred_element_type=jnp.float32)
    route_w = jnp.take_along_axis(jax.nn.softmax(logits, axis=-1), topk_idx, axis=1)
    shared_out = swiglu_rows(normed, shared_gate, shared_up, shared_down)
    flat_expert = topk_idx.reshape(-1)
    row_order = jnp.argsort(flat_expert, stable=True)
    sorted_expert = flat_expert[row_order]
    counts = jnp.zeros((EXPERTS,), jnp.int32).at[flat_expert].add(1)
    padded = (counts + ROW_BLOCK - 1) // ROW_BLOCK * ROW_BLOCK
    sorted_start = jnp.cumsum(counts) - counts
    padded_end = jnp.cumsum(padded)
    padded_start = padded_end - padded
    dest_sorted = padded_start[sorted_expert] + jnp.arange(ROUTE_ROWS) - sorted_start[sorted_expert]
    slot_token = jnp.full((NUM_BLOCKS * ROW_BLOCK,), NUM_TOKENS, jnp.int32).at[dest_sorted].set(row_order // TOP_K)
    dest_of_row = jnp.zeros((ROUTE_ROWS,), jnp.int32).at[row_order].set(dest_sorted)
    block_first = jnp.arange(NUM_BLOCKS) * ROW_BLOCK
    block_expert = jnp.minimum(jnp.sum(block_first[:, None] >= padded_end[None, :], axis=1), EXPERTS - 1)
    normed_pad = jnp.concatenate([normed, jnp.zeros((1, HIDDEN), normed.dtype)], axis=0)
    block_rows = normed_pad[slot_token].reshape(NUM_BLOCKS, ROW_BLOCK, HIDDEN)

    def one_block(block_in):
        block_x, expert_id = block_in
        expert_out = swiglu_rows(block_x, w_gate[expert_id], w_up[expert_id], w_down[expert_id])
        return expert_out.astype(jnp.bfloat16)

    padded_out = lax.map(one_block, (block_rows, block_expert)).reshape(NUM_BLOCKS * ROW_BLOCK, HIDDEN)
    row_out = padded_out[dest_of_row].reshape(NUM_TOKENS, TOP_K, HIDDEN)
    routed = jnp.sum(row_out.astype(jnp.float32) * route_w[:, :, None], axis=1)
    return (hidden.astype(jnp.float32) + shared_out + routed).astype(jnp.bfloat16)
```

```python
import functools

import jax
import jax.numpy as jnp
from jax import lax
from jax.experimental import pallas as pl
from jax.experimental.pallas import tpu as pltpu
from jax.sharding import PartitionSpec as P

NORM_EPS = 1e-6
MESH = pl.DeviceIdType.MESH
F32 = jnp.float32
BF16 = jnp.bfloat16

OWN, XN, YN, DG = 0, 1, 2, 3
SS_SLOT = {XN: 0, YN: 1, DG: 0, OWN: 1}
PEERS = [(q, r) for q in range(4) for r in range(2) if (q, r) != (0, 0)]


def dot(a, b):
    return jnp.dot(a, b, preferred_element_type=F32)


def moe_kernel(cfg, hid, gain, rw, topk, wg, wu, wd, sg, su, sd, out,
               gu, dn, g, rwp, wloc, win, rankm, x, act, o, comb, ash, acc, ss, sr, s, rx, ry, qx, qy,
               gu_sem, dn_sem, ag_s, ag_r, sib_s, sib_r, ici_s, ici_r):
    T, H, FF, EL, SLOT, NB, BW = cfg
    HT = T // 2
    me = lax.axis_index("ep")
    core, xx, yy = me % 2, (me // 2) % 2, me // 4

    def ep_of(q, r):
        nx = 1 - xx if q % 2 else xx
        ny = 1 - yy if q // 2 else yy
        nc = 1 - core if r else core
        return 4 * ny + 2 * nx + nc

    def rcopy(src, dst, send, recv, q, r):
        return pltpu.make_async_remote_copy(src_ref=src, dst_ref=dst, send_sem=send, recv_sem=recv,
                                            device_id={"ep": ep_of(q, r)}, device_id_type=MESH)

    lo, hi = pl.ds(0, HT), pl.ds(HT, HT)
    ag = {
        0: (g.at[OWN, 0], g.at[OWN, 1], OWN, 1),
        1: (g.at[OWN, 0, lo], g.at[XN, 0, lo], XN, 0),
        2: (g.at[OWN, 0, hi], g.at[YN, 0, hi], YN, 0),
        3: (g.at[OWN, 0, hi], g.at[XN, 0, hi], XN, 0),
        4: (g.at[OWN, 0, lo], g.at[YN, 0, lo], YN, 0),
        5: (g.at[XN, 0, lo], g.at[DG, 0, lo], YN, 0),
        6: (g.at[YN, 0, hi], g.at[DG, 0, hi], XN, 0),
        7: (g.at[XN, 0, lo], g.at[XN, 1, lo], OWN, 1),
        8: (g.at[YN, 0, hi], g.at[YN, 1, hi], OWN, 1),
        9: (g.at[XN, 0, hi], g.at[XN, 1, hi], OWN, 1),
        10: (g.at[YN, 0, lo], g.at[YN, 1, lo], OWN, 1),
        11: (g.at[DG, 0, lo], g.at[DG, 1, lo], OWN, 1),
        12: (g.at[DG, 0, hi], g.at[DG, 1, hi], OWN, 1),
    }
    for j, (q, r) in enumerate(PEERS):
        ag[13 + j] = (wloc.at[ep_of(q, r)], win.at[q, r], q, r)

    def agc(k):
        src, dst, q, r = ag[k]
        return rcopy(src, dst, ag_s.at[k], ag_r.at[k], q, r)

    def sibc(q, n):
        return rcopy(ss.at[SS_SLOT[q], n], sr.at[q, n], sib_s.at[q, n], sib_r.at[q, n], OWN, 1)

    def icic(k, n):
        src, dst, q = [
            (s.at[XN - 1, n, lo], rx.at[n, lo], XN),
            (s.at[YN - 1, n, hi], ry.at[n, hi], YN),
            (s.at[DG - 1, n, lo], qx.at[n], XN),
            (s.at[DG - 1, n, hi], qy.at[n], YN),
            (s.at[YN - 1, n, lo], ry.at[n, lo], YN),
            (s.at[XN - 1, n, hi], rx.at[n, hi], XN),
        ][k]
        return rcopy(src, dst, ici_s.at[k, n], ici_r.at[k, n], q, 0)

    def gu_loads(e, slot):
        return [pltpu.make_async_copy(wg.at[e], gu.at[slot, :, pl.ds(0, FF)], gu_sem.at[slot, 0]),
                pltpu.make_async_copy(wu.at[e], gu.at[slot, :, pl.ds(FF, FF)], gu_sem.at[slot, 1])]

    def dn_load(n, slot):
        return pltpu.make_async_copy(wd.at[:, :, pl.ds(pl.multiple_of(n * BW, BW), BW)], dn.at[slot], dn_sem.at[slot])

    def sd_load(n, slot):
        return pltpu.make_async_copy(sd.at[:, :, pl.ds(pl.multiple_of(n * BW, BW), BW)], dn.at[slot, pl.ds(0, 2)],
                                     dn_sem.at[slot])

    sg_load = pltpu.make_async_copy(sg, gu.at[2], gu_sem.at[2, 0])
    su_load = pltpu.make_async_copy(su, gu.at[3], gu_sem.at[3, 0])
    sg_load.start()
    su_load.start()
    sd_load(0, 0).start()
    sd_load(1, 1).start()
    for e in range(2):
        for c in gu_loads(e, e):
            c.start()

    barrier = pltpu.get_barrier_semaphore()
    for q, r in PEERS:
        pl.semaphore_signal(barrier, inc=1, device_id={"ep": ep_of(q, r)}, device_id_type=MESH)

    h = hid[...].astype(F32)
    inv = lax.rsqrt(jnp.mean(h * h, axis=-1, keepdims=True) + NORM_EPS)
    g[OWN, 0] = (h * inv * gain[...]).astype(BF16)
    pl.semaphore_wait(barrier, len(PEERS))
    for k in (1, 2, 0, 3, 4):
        agc(k).start()

    rwp[...] = jnp.zeros_like(rwp)
    rwp[:, 0:64] = rw[...]
    logits = dot(g[OWN, 0], rwp[...])
    lane = lax.broadcasted_iota(jnp.int32, logits.shape, 1)
    logits = jnp.where(lane < 64, logits, -jnp.inf)
    ex = jnp.exp(logits - jnp.max(logits, axis=-1, keepdims=True))
    p = ex / jnp.sum(ex, axis=-1, keepdims=True)
    chosen = topk[:, 0:1] == lane
    for j in range(1, topk.shape[1]):
        chosen = jnp.logical_or(chosen, topk[:, j:j + 1] == lane)
    wt = jnp.where(chosen, p, -1.0).T
    wloc[...] = wt[0:64].reshape(8, EL, T)
    for j in range(len(PEERS)):
        agc(13 + j).start()
    win[OWN, 0] = wloc[me]

    sg_load.wait()
    su_load.wait()

    @pl.loop(0, ash.shape[1] // BW)
    def _(n):
        cols = pl.ds(pl.multiple_of(n * BW, BW), BW)
        ga = dot(g[OWN, 0], gu[2, :, cols])
        up = dot(g[OWN, 0], gu[3, :, cols])
        ash[:, cols] = (jax.nn.silu(ga) * up).astype(BF16)

    for e in (2, 3):
        for c in gu_loads(e, e):
            c.start()

    agc(1).wait_recv()
    agc(5).start()
    agc(7).start()
    agc(2).wait_recv()
    agc(6).start()
    agc(8).start()

    @pl.loop(0, NB)
    def _(n):
        cols = pl.ds(pl.multiple_of(n * BW, BW), BW)
        slot = n % 2
        sd_load(n, slot).wait()
        acc[n] = hid[:, cols].astype(F32) + dot(ash[...], dn[slot, 0:2].reshape(2 * FF, BW))

        @pl.when(n + 2 < NB)
        def _():
            sd_load(n + 2, slot).start()

        @pl.when(n + 2 >= NB)
        def _():
            dn_load(n + 2 - NB, slot).start()

    for j in range(len(PEERS)):
        agc(13 + j).wait_recv()
    wall = win[...].reshape(8 * EL, T)
    upper = (lax.broadcasted_iota(jnp.int32, (T, T), 0) < lax.broadcasted_iota(jnp.int32, (T, T), 1))
    upper = jnp.where(upper, 1.0, 0.0).astype(BF16)
    rank = dot(jnp.where(wall >= 0, 1.0, 0.0).astype(BF16), upper)
    rankm[...] = jnp.where(wall >= 0, rank, -1.0).reshape(4, 2, EL, T)

    def dispatch(q, r, i):
        rk = rankm[q, r]
        w = win[q, r]
        slot_id = lax.broadcasted_iota(jnp.int32, (EL, SLOT, T), 1).astype(F32)
        hit = jnp.broadcast_to(rk[:, None, :], (EL, SLOT, T)) == slot_id
        pick = jnp.where(hit, 1.0, 0.0).reshape(EL * SLOT, T).astype(BF16)
        x[:, i] = dot(pick, g[q, r]).astype(BF16).reshape(EL, SLOT, H)
        cw = jnp.where(hit, jnp.broadcast_to(w[:, None, :], (EL, SLOT, T)), 0.0).reshape(EL * SLOT, T).T
        c1 = cw.astype(BF16)
        rest = cw - c1.astype(F32)
        c2 = rest.astype(BF16)
        comb[i, 0] = c1
        comb[i, 1] = c2
        comb[i, 2] = (rest - c2.astype(F32)).astype(BF16)

    def finish(q, n):
        sibc(q, n).wait_recv()
        if q == OWN:
            acc[n] = acc[n] + sr[q, n]
            return
        s[q - 1, n] = s[q - 1, n] + sr[q, n]
        if q == XN:
            icic(0, n).start()
        elif q == YN:
            icic(1, n).start()
        else:
            icic(2, n).start()
            icic(3, n).start()

    def relay(n):
        icic(2, n).wait_recv()
        s[YN - 1, n, lo] = s[YN - 1, n, lo] + qx[n]
        icic(4, n).start()
        icic(3, n).wait_recv()
        s[XN - 1, n, hi] = s[XN - 1, n, hi] + qy[n]
        icic(5, n).start()

    def expert_pass(p, chips, down_first, between, mid_steps):
        owners = 2 * len(chips)
        rows = owners * SLOT

        @pl.loop(0, owners)
        def _(i):
            dispatch(chips[0] + i // 2, i % 2, i)

        @pl.loop(0, EL)
        def _(i):
            e = EL - 1 - i if p == 1 else i
            slot = e % 4
            fresh = (e >= 0) if p == 0 else ((e < 4) if p == 1 else (e >= 4))

            @pl.when(fresh)
            def _():
                for c in gu_loads(e, slot):
                    c.wait()

            xe = x[e, 0:owners].reshape(rows, H)
            gua = dot(xe, gu[slot])
            act[e, 0:rows] = (jax.nn.silu(gua[:, 0:FF]) * gua[:, FF:2 * FF]).astype(BF16)

            @pl.when(i < 4)
            def _():
                nxt = e - 4 if p == 1 else e + 4
                for c in gu_loads(nxt, slot):
                    c.start()

            mid_steps(i)

        between()

        @pl.loop(0, NB)
        def _(n):
            slot = (n + NB * (p + 1)) % 2
            dn_load(n, slot).wait()
            for e in range(EL):
                res = dot(act[e, 0:rows], dn[slot, e]).astype(BF16)
                o[0:owners, e] = res.reshape(owners, SLOT, BW)

            @pl.when(jnp.logical_or(n + 2 < NB, p < 2))
            def _():
                dn_load((n + 2) % NB, slot).start()

            for i in sorted(range(owners), key=lambda i: -(i % 2)):
                q = chips[i // 2]
                oo = o[i].reshape(EL * SLOT, BW)
                part = dot(comb[i, 0], oo) + dot(comb[i, 1], oo) + dot(comb[i, 2], oo)
                if i % 2:
                    if p == 1:
                        sibc(XN, n).wait_send()
                    elif p == 2:
                        sibc(YN, n).wait_send()
                    ss[SS_SLOT[q], n] = part
                    sibc(q, n).start()
                elif q == OWN:
                    acc[n] = acc[n] + part
                else:
                    s[q - 1, n] = part

            @pl.when(n > 0)
            def _():
                for q in chips:
                    finish(q, n - 1)

            down_first(n)

        for q in chips:
            finish(q, NB - 1)

    nothing = lambda *a: None

    agc(3).wait_recv()
    agc(9).start()
    agc(4).wait_recv()
    agc(10).start()
    for k in (7, 8, 9, 10):
        agc(k).wait_recv()

    def forward_diag():
        agc(5).wait_recv()
        agc(11).start()
        agc(6).wait_recv()
        agc(12).start()

    expert_pass(0, [XN, YN], nothing, forward_diag, nothing)

    agc(11).wait_recv()
    agc(12).wait_recv()
    expert_pass(1, [DG], nothing, nothing, nothing)

    agc(0).wait_recv()

    def relay_gu(i):
        @pl.when(i % 3 == 1)
        def _():
            relay(i // 3)

    def relay_dn(n):
        @pl.when(n == 1)
        def _():
            relay(3)

        @pl.when(n == 4)
        def _():
            relay(4)

    expert_pass(2, [OWN], relay_dn, nothing, relay_gu)

    for n in range(NB):
        for k in (0, 5, 1, 4):
            icic(k, n).wait_recv()
        out[:, n * BW:(n + 1) * BW] = (acc[n] + rx[n] + ry[n]).astype(BF16)

    for k in range(13 + len(PEERS)):
        agc(k).wait_send()
    for n in range(NB):
        for q in (DG, OWN):
            sibc(q, n).wait_send()
        for k in range(6):
            icic(k, n).wait_send()


def solution(mesh):
    def local_step(hidden, norm_gain, router_w, topk_idx, w_gate, w_up, w_down, shared_gate, shared_up, shared_down):
        T, H = hidden.shape
        EL, _, FF = w_gate.shape
        BW = 256
        NB = H // BW
        SLOT = 48
        cfg = (T, H, FF, EL, SLOT, NB, BW)
        vm = pl.BlockSpec(memory_space=pltpu.VMEM)
        anym = pl.BlockSpec(memory_space=pl.ANY)
        dma = pltpu.SemaphoreType.DMA
        n_ag = 13 + len(PEERS)
        return pl.pallas_call(
            functools.partial(moe_kernel, cfg),
            out_shape=jax.ShapeDtypeStruct((T, H), BF16),
            in_specs=[vm, vm, vm, vm] + [anym] * 6,
            out_specs=vm,
            scratch_shapes=[
                pltpu.VMEM((4, H, 2 * FF), BF16),
                pltpu.VMEM((2, EL, FF, BW), BF16),
                pltpu.VMEM((4, 2, T, H), BF16),
                pltpu.VMEM((H, 128), BF16),
                pltpu.VMEM((8, EL, T), F32),
                pltpu.VMEM((4, 2, EL, T), F32),
                pltpu.VMEM((4, 2, EL, T), F32),
                pltpu.VMEM((EL, 4, SLOT, H), BF16),
                pltpu.VMEM((EL, 4 * SLOT, FF), BF16),
                pltpu.VMEM((4, EL, SLOT, BW), BF16),
                pltpu.VMEM((4, 3, T, EL * SLOT), BF16),
                pltpu.VMEM((T, 2 * FF), BF16),
                pltpu.VMEM((NB, T, BW), F32),
                pltpu.VMEM((2, NB, T, BW), F32),
                pltpu.VMEM((4, NB, T, BW), F32),
                pltpu.VMEM((3, NB, T, BW), F32),
                pltpu.VMEM((NB, T, BW), F32),
                pltpu.VMEM((NB, T, BW), F32),
                pltpu.VMEM((NB, T // 2, BW), F32),
                pltpu.VMEM((NB, T // 2, BW), F32),
                dma((4, 2)), dma((2,)),
                dma((n_ag,)), dma((n_ag,)), dma((4, NB)), dma((4, NB)), dma((6, NB)), dma((6, NB)),
            ],
            compiler_params=pltpu.CompilerParams(collective_id=0, has_side_effects=True, vmem_limit_bytes=67043328),
            name="moe_block",
        )(hidden, norm_gain.reshape(1, H), router_w, topk_idx, w_gate, w_up, w_down, shared_gate, shared_up,
          shared_down.reshape(2, FF, H))

    token_spec = P(('dp', 'ep'), None)
    expert_spec = P('ep', None, None)
    return jax.shard_map(
        local_step,
        mesh=mesh,
        in_specs=(token_spec, P(None), P(None, None), token_spec, expert_spec, expert_spec, expert_spec,
                  P(None, None), P(None, None), P(None, None)),
        out_specs=token_spec,
        check_vma=False,
    )
```

```python
import functools

import jax
import jax.numpy as jnp
from jax import lax
from jax.experimental import pallas as pl
from jax.experimental.pallas import tpu as pltpu
from jax.sharding import PartitionSpec as P

NORM_EPS = 1e-6
MESH = pl.DeviceIdType.MESH
F32 = jnp.float32
BF16 = jnp.bfloat16

OWN, XN, YN, DG = 0, 1, 2, 3
SR_SLOT = {XN: 0, YN: 1, DG: 2, OWN: 0}
SS_SLOT = {XN: 0, YN: 1, DG: 0, OWN: 1}
NAG = 10
PEERS = [(q, r) for q in range(4) for r in range(2) if (q, r) != (0, 0)]


def dot(a, b):
    return jnp.dot(a, b, preferred_element_type=F32)


def moe_kernel(cfg, hid, gain, rwt, topkt, wg, wu, wd, sg, su, sd, out,
               gu, dn, g, wloc, win, rankm, x, act, o, comb, ash, acc, ss, sr, s, rx, ry, qx, qy,
               gu_sem, dn_sem, ag_s, ag_r, sib_s, sib_r, ici_s, ici_r):
    T, H, FF, EL, SLOT, NB, BW, NS = cfg
    HT = T // 2
    me = lax.axis_index("ep")
    core, xx, yy = me % 2, (me // 2) % 2, me // 4

    def ep_of(q, r):
        return 4 * ((yy + q // 2) % 2) + 2 * ((xx + q % 2) % 2) + (core + r) % 2

    def rcopy(src, dst, send, recv, q, r):
        return pltpu.make_async_remote_copy(src_ref=src, dst_ref=dst, send_sem=send, recv_sem=recv,
                                            device_id={"ep": ep_of(q, r)}, device_id_type=MESH)

    lo, hi = pl.ds(0, HT), pl.ds(HT, HT)
    qa, qb = 1 + core, 2 - core
    ha = pl.ds(pl.multiple_of(core * HT, HT), HT)
    hb = pl.ds(pl.multiple_of((1 - core) * HT, HT), HT)
    ag = {
        0: (g.at[OWN, 0], g.at[OWN, 1], OWN, 1),
        1: (g.at[OWN, 0, lo], g.at[qa, 0, lo], qa, 0),
        2: (g.at[OWN, 0, hi], g.at[qa, 0, hi], qa, 0),
        3: (g.at[OWN, 0], g.at[qb, 0], qb, 0),
        4: (g.at[qa, 0, ha], g.at[DG, 0, ha], qb, 0),
        5: (g.at[qb, 0, hb], g.at[DG, 0, hb], qa, 0),
        6: (g.at[qa, 0], g.at[qa, 1], OWN, 1),
        7: (g.at[qb, 0], g.at[qb, 1], OWN, 1),
        8: (g.at[DG, 0, ha], g.at[DG, 1, ha], OWN, 1),
        9: (g.at[DG, 0, hb], g.at[DG, 1, hb], OWN, 1),
    }
    for j, (q, r) in enumerate(PEERS):
        ag[NAG + j] = (wloc.at[ep_of(q, r)], win.at[q, r], q, r)

    def agc(k):
        src, dst, q, r = ag[k]
        return rcopy(src, dst, ag_s.at[k], ag_r.at[k], q, r)

    def sibc(q, n):
        return rcopy(ss.at[SS_SLOT[q], n], sr.at[SR_SLOT[q], n], sib_s.at[q, n], sib_r.at[q, n], OWN, 1)

    def icic(k, n):
        src, dst, q = [
            (s.at[XN - 1, n, lo], rx.at[n, lo], XN),
            (s.at[YN - 1, n, hi], ry.at[n, hi], YN),
            (s.at[DG - 1, n, lo], qx.at[n], XN),
            (s.at[DG - 1, n, hi], qy.at[n], YN),
            (s.at[YN - 1, n, lo], ry.at[n, lo], YN),
            (s.at[XN - 1, n, hi], rx.at[n, hi], XN),
        ][k]
        return rcopy(src, dst, ici_s.at[k, n], ici_r.at[k, n], q, 0)

    def gu_loads(e, slot):
        return [pltpu.make_async_copy(wg.at[e], gu.at[slot, :, pl.ds(0, FF)], gu_sem.at[slot, 0]),
                pltpu.make_async_copy(wu.at[e], gu.at[slot, :, pl.ds(FF, FF)], gu_sem.at[slot, 1])]

    def dn_load(n, slot):
        return pltpu.make_async_copy(wd.at[:, :, pl.ds(pl.multiple_of(n * BW, BW), BW)], dn.at[slot], dn_sem.at[slot])

    def sd_load(n, slot):
        return pltpu.make_async_copy(sd.at[:, :, pl.ds(pl.multiple_of(n * BW, BW), BW)], dn.at[slot, pl.ds(0, 2)],
                                     dn_sem.at[slot])

    sg_load = pltpu.make_async_copy(sg, gu.at[NS - 2], gu_sem.at[NS - 2, 0])
    su_load = pltpu.make_async_copy(su, gu.at[NS - 1], gu_sem.at[NS - 1, 0])
    sg_load.start()
    su_load.start()
    sd_load(0, 0).start()
    sd_load(1, 1).start()
    for e in range(NS - 2):
        for c in gu_loads(e, e):
            c.start()

    barrier = pltpu.get_barrier_semaphore()
    for q, r in PEERS:
        pl.semaphore_signal(barrier, inc=1, device_id={"ep": ep_of(q, r)}, device_id_type=MESH)

    h = hid[...].astype(F32)
    inv = lax.rsqrt(jnp.mean(h * h, axis=-1, keepdims=True) + NORM_EPS)
    g[OWN, 0] = (h * inv * gain[...][None, :]).astype(BF16)
    pl.semaphore_wait(barrier, len(PEERS))
    agc(1).start()
    agc(0).start()

    logits = lax.dot_general(rwt[...], g[OWN, 0], (((1,), (1,)), ((), ())), preferred_element_type=F32)
    ex = jnp.exp(logits - jnp.max(logits, axis=0, keepdims=True))
    p = ex / jnp.sum(ex, axis=0, keepdims=True)
    expert = lax.broadcasted_iota(jnp.int32, logits.shape, 0)
    chosen = topkt[0:1, :] == expert
    for j in range(1, topkt.shape[0]):
        chosen = jnp.logical_or(chosen, topkt[j:j + 1, :] == expert)
    wloc[...] = jnp.where(chosen, p, -1.0).reshape(8, EL, T)
    for j in range(len(PEERS)):
        agc(NAG + j).start()
    agc(2).start()
    win[OWN, 0] = wloc[me]

    sg_load.wait()
    su_load.wait()

    @pl.loop(0, ash.shape[1] // BW)
    def _(n):
        cols = pl.ds(pl.multiple_of(n * BW, BW), BW)
        ga = dot(g[OWN, 0], gu[NS - 2, :, cols])
        up = dot(g[OWN, 0], gu[NS - 1, :, cols])
        ash[:, cols] = (jax.nn.silu(ga) * up).astype(BF16)

    for e in (NS - 2, NS - 1):
        for c in gu_loads(e, e):
            c.start()

    @pl.loop(0, NB)
    def _(n):
        cols = pl.ds(pl.multiple_of(n * BW, BW), BW)
        slot = n % 2
        sd_load(n, slot).wait()
        acc[n] = hid[:, cols].astype(F32) + dot(ash[...], dn[slot, 0:2].reshape(2 * FF, BW))

        @pl.when(n + 2 < NB)
        def _():
            sd_load(n + 2, slot).start()

        @pl.when(n + 2 >= NB)
        def _():
            dn_load(n + 2 - NB, slot).start()

    agc(1).wait_send()
    agc(2).wait_send()
    agc(3).start()
    agc(1).wait_recv()
    agc(2).wait_recv()
    agc(6).start()
    agc(4).start()

    for j in range(len(PEERS)):
        agc(NAG + j).wait_recv()
    wall = win[...].reshape(8 * EL, T)
    upper = (lax.broadcasted_iota(jnp.int32, (T, T), 0) < lax.broadcasted_iota(jnp.int32, (T, T), 1))
    upper = jnp.where(upper, 1.0, 0.0).astype(BF16)
    rank = dot(jnp.where(wall >= 0, 1.0, 0.0).astype(BF16), upper)
    rankm[...] = jnp.where(wall >= 0, rank, -1.0).reshape(4, 2, EL, T)

    def hits(q, r):
        slot_id = lax.broadcasted_iota(jnp.int32, (EL, SLOT, T), 1).astype(F32)
        return jnp.broadcast_to(rankm[q, r][:, None, :], (EL, SLOT, T)) == slot_id

    def dispatch(q, r, i):
        pick = jnp.where(hits(q, r), 1.0, 0.0).reshape(EL * SLOT, T).astype(BF16)
        x[:, i] = dot(pick, g[q, r]).astype(BF16).reshape(EL, SLOT, H)

    def build_comb(q, r, i):
        w = jnp.broadcast_to(win[q, r][:, None, :], (EL, SLOT, T))
        cw = jnp.where(hits(q, r), w, 0.0).reshape(EL * SLOT, T).T
        c1 = cw.astype(BF16)
        rest = cw - c1.astype(F32)
        c2 = rest.astype(BF16)
        comb[i, 0] = c1
        comb[i, 1] = c2
        comb[i, 2] = (rest - c2.astype(F32)).astype(BF16)

    def finish(q, n):
        sibc(q, n).wait_recv()
        if q == OWN:
            acc[n] = acc[n] + sr[SR_SLOT[q], n]
            return
        s[q - 1, n] = s[q - 1, n] + sr[SR_SLOT[q], n]
        if q == XN:
            icic(0, n).start()
        elif q == YN:
            icic(1, n).start()
        else:
            icic(2, n).start()
            icic(3, n).start()

    def relay(n):
        icic(2, n).wait_recv()
        s[YN - 1, n, lo] = s[YN - 1, n, lo] + qx[n]
        icic(4, n).start()
        icic(3, n).wait_recv()
        s[XN - 1, n, hi] = s[XN - 1, n, hi] + qy[n]
        icic(5, n).start()

    def gate_up(p, a0, a1, step):
        @pl.loop(0, EL)
        def _(i):
            e = EL - 1 - i if p % 2 else i
            slot = e % NS

            @pl.when(i >= (NS if p else 0))
            def _():
                for c in gu_loads(e, slot):
                    c.wait()

            gua = dot(x[e].reshape(2 * SLOT, H), gu[slot])
            res = (jax.nn.silu(gua[:, 0:FF]) * gua[:, FF:2 * FF]).astype(BF16)
            act[e, a0] = res[0:SLOT]
            act[e, a1] = res[SLOT:2 * SLOT]

            @pl.when(i < EL - NS)
            def _():
                for c in gu_loads(e - NS if p % 2 else e + NS, slot):
                    c.start()

            step(i)

    def down(p, chips, step):
        owners = 2 * len(chips)

        @pl.loop(0, NB)
        def _(n):
            slot = (n + NB * (p + 1)) % 2
            dn_load(n, slot).wait()
            for e in range(EL):
                res = dot(act[e, 0:owners].reshape(owners * SLOT, FF), dn[slot, e]).astype(BF16)
                o[0:owners, e] = res.reshape(owners, SLOT, BW)

            @pl.when(jnp.logical_or(n + 2 < NB, p < 2))
            def _():
                dn_load((n + 2) % NB, slot).start()

            for i in sorted(range(owners), key=lambda i: -(i % 2)):
                q = chips[i // 2]
                oo = o[i].reshape(EL * SLOT, BW)
                part = dot(comb[i, 0], oo) + dot(comb[i, 1], oo) + dot(comb[i, 2], oo)
                if i % 2:
                    if p:
                        sibc(XN if p == 1 else YN, n).wait_send()
                    ss[SS_SLOT[q], n] = part
                    sibc(q, n).start()
                elif q == OWN:
                    acc[n] = acc[n] + part
                else:
                    s[q - 1, n] = part

            @pl.when(n > 0)
            def _():
                for q in chips:
                    finish(q, n - 1)

            step(n)

        for q in chips:
            finish(q, NB - 1)

    nothing = lambda i: None

    @pl.loop(0, 4)
    def _(i):
        build_comb(1 + i // 2, i % 2, i)

    def second_arrival(i):
        @pl.when(i == 6)
        def _():
            agc(3).wait_recv()
            agc(7).start()
            agc(5).start()

    agc(6).wait_recv()
    dispatch(qa, 0, 0)
    dispatch(qb, 1, 1)
    gate_up(0, 2 * (qa - 1), 2 * (qb - 1) + 1, second_arrival)
    agc(7).wait_recv()
    dispatch(qb, 0, 0)
    dispatch(qa, 1, 1)
    gate_up(1, 2 * (qb - 1), 2 * (qa - 1) + 1, nothing)
    agc(4).wait_recv()
    agc(8).start()
    agc(5).wait_recv()
    agc(9).start()
    down(0, [XN, YN], nothing)

    for r in range(2):
        build_comb(DG, r, r)
    agc(8).wait_recv()
    agc(9).wait_recv()
    for r in range(2):
        dispatch(DG, r, r)
    gate_up(2, 0, 1, nothing)
    down(1, [DG], nothing)

    def relay_gu(i):
        @pl.when(i % 3 == 1)
        def _():
            relay(i // 3)

    def relay_dn(n):
        @pl.when(n == 1)
        def _():
            relay(3)

        @pl.when(n == 4)
        def _():
            relay(4)

    agc(0).wait_recv()
    for r in range(2):
        build_comb(OWN, r, r)
        dispatch(OWN, r, r)
    gate_up(3, 0, 1, relay_gu)
    down(2, [OWN], relay_dn)

    for n in range(NB):
        for k in (0, 5, 1, 4):
            icic(k, n).wait_recv()
        out[:, n * BW:(n + 1) * BW] = (acc[n] + rx[n] + ry[n]).astype(BF16)

    for k in range(NAG + len(PEERS)):
        if k not in (1, 2):
            agc(k).wait_send()
    for n in range(NB):
        for q in (DG, OWN):
            sibc(q, n).wait_send()
        for k in range(6):
            icic(k, n).wait_send()


def solution(mesh):
    def local_step(hidden, norm_gain, router_w, topk_idx, w_gate, w_up, w_down, shared_gate, shared_up, shared_down):
        T, H = hidden.shape
        EL, _, FF = w_gate.shape
        BW = 256
        NB = H // BW
        SLOT = 48
        NS = 5
        cfg = (T, H, FF, EL, SLOT, NB, BW, NS)
        vm = pl.BlockSpec(memory_space=pltpu.VMEM)
        anym = pl.BlockSpec(memory_space=pl.ANY)
        dma = pltpu.SemaphoreType.DMA
        n_ag = NAG + len(PEERS)
        return pl.pallas_call(
            functools.partial(moe_kernel, cfg),
            out_shape=jax.ShapeDtypeStruct((T, H), BF16),
            in_specs=[vm, vm, vm, vm] + [anym] * 6,
            out_specs=vm,
            scratch_shapes=[
                pltpu.VMEM((NS, H, 2 * FF), BF16),
                pltpu.VMEM((2, EL, FF, BW), BF16),
                pltpu.VMEM((4, 2, T, H), BF16),
                pltpu.VMEM((8, EL, T), F32),
                pltpu.VMEM((4, 2, EL, T), F32),
                pltpu.VMEM((4, 2, EL, T), F32),
                pltpu.VMEM((EL, 2, SLOT, H), BF16),
                pltpu.VMEM((EL, 4, SLOT, FF), BF16),
                pltpu.VMEM((4, EL, SLOT, BW), BF16),
                pltpu.VMEM((4, 3, T, EL * SLOT), BF16),
                pltpu.VMEM((T, 2 * FF), BF16),
                pltpu.VMEM((NB, T, BW), F32),
                pltpu.VMEM((2, NB, T, BW), F32),
                pltpu.VMEM((3, NB, T, BW), F32),
                pltpu.VMEM((3, NB, T, BW), F32),
                pltpu.VMEM((NB, T, BW), F32),
                pltpu.VMEM((NB, T, BW), F32),
                pltpu.VMEM((NB, T // 2, BW), F32),
                pltpu.VMEM((NB, T // 2, BW), F32),
                dma((NS, 2)), dma((2,)),
                dma((n_ag,)), dma((n_ag,)), dma((4, NB)), dma((4, NB)), dma((6, NB)), dma((6, NB)),
            ],
            compiler_params=pltpu.CompilerParams(collective_id=0, has_side_effects=True, vmem_limit_bytes=67043328),
            name="moe_block",
        )(hidden, norm_gain, router_w.T, topk_idx.T, w_gate, w_up, w_down, shared_gate, shared_up,
          shared_down.reshape(2, FF, H))

    token_spec = P(('dp', 'ep'), None)
    expert_spec = P('ep', None, None)
    return jax.shard_map(
        local_step,
        mesh=mesh,
        in_specs=(token_spec, P(None), P(None, None), token_spec, expert_spec, expert_spec, expert_spec,
                  P(None, None), P(None, None), P(None, None)),
        out_specs=token_spec,
        check_vma=False,
    )
```

```python
import functools

import jax
import jax.numpy as jnp
from jax import lax
from jax.experimental import pallas as pl
from jax.experimental.pallas import tpu as pltpu
from jax.sharding import PartitionSpec as P

NORM_EPS = 1e-6
MESH = pl.DeviceIdType.MESH
F32 = jnp.float32
BF16 = jnp.bfloat16

OWN, XN, YN, DG = 0, 1, 2, 3
SR_SLOT = {XN: 0, YN: 1, DG: 2, OWN: 0}
SS_SLOT = {XN: 0, YN: 1, DG: 0, OWN: 1}
NAG = 13
PEERS = [(q, r) for q in range(4) for r in range(2) if (q, r) != (0, 0)]


def dot(a, b):
    return jnp.dot(a, b, preferred_element_type=F32)


def moe_kernel(cfg, hid, gain, rwt, topkt, wg, wu, wd, sg, su, sd, out,
               gu, dn, g, wloc, win, rankm, x, act, o, comb, ash, acc, ss, sr, s, rx, ry, qx, qy, fin,
               gu_sem, dn_sem, out_sem, ag_s, ag_r, sib_s, sib_r, ici_s, ici_r):
    T, H, FF, EL, SLOT, NB, BW, NS = cfg
    HT = T // 2
    me = lax.axis_index("ep")
    core, xx, yy = me % 2, (me // 2) % 2, me // 4

    def ep_of(q, r):
        return 4 * ((yy + q // 2) % 2) + 2 * ((xx + q % 2) % 2) + (core + r) % 2

    def rcopy(src, dst, send, recv, q, r):
        return pltpu.make_async_remote_copy(src_ref=src, dst_ref=dst, send_sem=send, recv_sem=recv,
                                            device_id={"ep": ep_of(q, r)}, device_id_type=MESH)

    lo, hi = pl.ds(0, HT), pl.ds(HT, HT)
    ag = {
        0: (g.at[OWN, 0], g.at[OWN, 1], OWN, 1),
        1: (g.at[OWN, 0, lo], g.at[XN, 0, lo], XN, 0),
        2: (g.at[OWN, 0, hi], g.at[YN, 0, hi], YN, 0),
        3: (g.at[OWN, 0, hi], g.at[XN, 0, hi], XN, 0),
        4: (g.at[OWN, 0, lo], g.at[YN, 0, lo], YN, 0),
        5: (g.at[XN, 0, lo], g.at[DG, 0, lo], YN, 0),
        6: (g.at[YN, 0, hi], g.at[DG, 0, hi], XN, 0),
        7: (g.at[XN, 0, lo], g.at[XN, 1, lo], OWN, 1),
        8: (g.at[YN, 0, hi], g.at[YN, 1, hi], OWN, 1),
        9: (g.at[XN, 0, hi], g.at[XN, 1, hi], OWN, 1),
        10: (g.at[YN, 0, lo], g.at[YN, 1, lo], OWN, 1),
        11: (g.at[DG, 0, lo], g.at[DG, 1, lo], OWN, 1),
        12: (g.at[DG, 0, hi], g.at[DG, 1, hi], OWN, 1),
    }
    for j, (q, r) in enumerate(PEERS):
        ag[NAG + j] = (wloc.at[ep_of(q, r)], win.at[q, r], q, r)

    def agc(k):
        src, dst, q, r = ag[k]
        return rcopy(src, dst, ag_s.at[k], ag_r.at[k], q, r)

    def sibc(q, n):
        return rcopy(ss.at[SS_SLOT[q], n], sr.at[SR_SLOT[q], n], sib_s.at[q, n], sib_r.at[q, n], OWN, 1)

    def icic(k, n):
        src, dst, q = [
            (s.at[XN - 1, n, lo], rx.at[n, lo], XN),
            (s.at[YN - 1, n, hi], ry.at[n, hi], YN),
            (s.at[DG - 1, n, lo], qx.at[n], XN),
            (s.at[DG - 1, n, hi], qy.at[n], YN),
            (s.at[YN - 1, n, lo], ry.at[n, lo], YN),
            (s.at[XN - 1, n, hi], rx.at[n, hi], XN),
        ][k]
        return rcopy(src, dst, ici_s.at[k, n], ici_r.at[k, n], q, 0)

    def gu_loads(e, slot):
        return [pltpu.make_async_copy(wg.at[e], gu.at[slot, :, pl.ds(0, FF)], gu_sem.at[slot, 0]),
                pltpu.make_async_copy(wu.at[e], gu.at[slot, :, pl.ds(FF, FF)], gu_sem.at[slot, 1])]

    def dn_load(n, slot):
        return pltpu.make_async_copy(wd.at[:, :, pl.ds(pl.multiple_of(n * BW, BW), BW)], dn.at[slot], dn_sem.at[slot])

    def sd_load(n, slot):
        return pltpu.make_async_copy(sd.at[:, :, pl.ds(pl.multiple_of(n * BW, BW), BW)], dn.at[slot, pl.ds(0, 2)],
                                     dn_sem.at[slot])

    def out_copy(n):
        cols = pl.ds(n * BW, BW)
        return pltpu.make_async_copy(fin.at[:, cols], out.at[:, cols], out_sem.at[n])

    sg_load = pltpu.make_async_copy(sg, gu.at[NS - 2], gu_sem.at[NS - 2, 0])
    su_load = pltpu.make_async_copy(su, gu.at[NS - 1], gu_sem.at[NS - 1, 0])
    sg_load.start()
    su_load.start()
    sd_load(0, 0).start()
    sd_load(1, 1).start()

    barrier = pltpu.get_barrier_semaphore()
    for q, r in PEERS:
        pl.semaphore_signal(barrier, inc=1, device_id={"ep": ep_of(q, r)}, device_id_type=MESH)

    h = hid[...].astype(F32)
    inv = lax.rsqrt(jnp.mean(h * h, axis=-1, keepdims=True) + NORM_EPS)
    g[OWN, 0] = (h * inv * gain[...][None, :]).astype(BF16)

    logits = lax.dot_general(rwt[...], g[OWN, 0], (((1,), (1,)), ((), ())), preferred_element_type=F32)
    ex = jnp.exp(logits - jnp.max(logits, axis=0, keepdims=True))
    p = ex / jnp.sum(ex, axis=0, keepdims=True)
    expert = lax.broadcasted_iota(jnp.int32, logits.shape, 0)
    chosen = topkt[0:1, :] == expert
    for j in range(1, topkt.shape[0]):
        chosen = jnp.logical_or(chosen, topkt[j:j + 1, :] == expert)
    wloc[...] = jnp.where(chosen, p, -1.0).reshape(8, EL, T)
    pl.semaphore_wait(barrier, len(PEERS))
    agc(1).start()
    agc(2).start()
    for j in range(len(PEERS)):
        agc(NAG + j).start()
    for k in (0, 3, 4):
        agc(k).start()
    win[OWN, 0] = wloc[me]

    sg_load.wait()
    su_load.wait()
    for e in range(NS - 2):
        for c in gu_loads(e, e):
            c.start()

    @pl.loop(0, ash.shape[1] // BW)
    def _(n):
        cols = pl.ds(pl.multiple_of(n * BW, BW), BW)
        ga = dot(g[OWN, 0], gu[NS - 2, :, cols])
        up = dot(g[OWN, 0], gu[NS - 1, :, cols])
        ash[:, cols] = (jax.nn.silu(ga) * up).astype(BF16)

    for e in (NS - 2, NS - 1):
        for c in gu_loads(e, e):
            c.start()

    @pl.loop(0, NB)
    def _(n):
        cols = pl.ds(pl.multiple_of(n * BW, BW), BW)
        slot = n % 2
        sd_load(n, slot).wait()
        acc[n] = hid[:, cols].astype(F32) + dot(ash[...], dn[slot, 0:2].reshape(2 * FF, BW))

        @pl.when(n + 2 < NB)
        def _():
            sd_load(n + 2, slot).start()

        @pl.when(n + 2 >= NB)
        def _():
            dn_load(n + 2 - NB, slot).start()

    for j in range(len(PEERS)):
        agc(NAG + j).wait_recv()
    wall = win[...].reshape(8 * EL, T)
    upper = (lax.broadcasted_iota(jnp.int32, (T, T), 0) < lax.broadcasted_iota(jnp.int32, (T, T), 1))
    upper = jnp.where(upper, 1.0, 0.0).astype(BF16)
    rank = dot(jnp.where(wall >= 0, 1.0, 0.0).astype(BF16), upper)
    rankm[...] = jnp.where(wall >= 0, rank, -1.0).reshape(4, 2, EL, T)

    def hits(q, r):
        slot_id = lax.broadcasted_iota(jnp.int32, (EL, SLOT, T), 1).astype(F32)
        return jnp.broadcast_to(rankm[q, r][:, None, :], (EL, SLOT, T)) == slot_id

    def dispatch(q, r, i):
        pick = jnp.where(hits(q, r), 1.0, 0.0).reshape(EL * SLOT, T).astype(BF16)
        x[:, pl.ds(pl.multiple_of(i * SLOT, SLOT), SLOT)] = dot(pick, g[q, r]).reshape(EL, SLOT, H)

    def build_comb(q, r, i):
        w = jnp.broadcast_to(win[q, r][:, None, :], (EL, SLOT, T))
        cw = jnp.where(hits(q, r), w, 0.0).reshape(EL * SLOT, T)
        c1 = cw.astype(BF16).astype(F32)
        c2 = (cw - c1).astype(BF16).astype(F32)
        comb[i] = jnp.concatenate([c1, c2, cw - c1 - c2], axis=0).T.astype(BF16)

    def finish(q, n):
        sibc(q, n).wait_recv()
        if q == OWN:
            acc[n] = acc[n] + sr[SR_SLOT[q], n]
            return
        s[q - 1, n] = s[q - 1, n] + sr[SR_SLOT[q], n]
        if q == XN:
            icic(0, n).start()
        elif q == YN:
            icic(1, n).start()
        else:
            icic(2, n).start()
            icic(3, n).start()

    def relay(n):
        icic(2, n).wait_recv()
        s[YN - 1, n, lo] = s[YN - 1, n, lo] + qx[n]
        icic(4, n).start()
        icic(3, n).wait_recv()
        s[XN - 1, n, hi] = s[XN - 1, n, hi] + qy[n]
        icic(5, n).start()

    def gate_up(p, chips, step):
        rows = 2 * len(chips) * SLOT

        @pl.loop(0, EL, unroll=2)
        def _(i):
            e = EL - 1 - i if p % 2 else i
            slot = e % NS

            @pl.when(i >= (NS if p else 0))
            def _():
                for c in gu_loads(e, slot):
                    c.wait()

            gua = dot(x[e, 0:rows].astype(BF16), gu[slot])
            act[e, 0:rows] = (jax.nn.silu(gua[:, 0:FF]) * gua[:, FF:2 * FF]).astype(BF16)

            @pl.when(i < EL - NS)
            def _():
                for c in gu_loads(e - NS if p % 2 else e + NS, slot):
                    c.start()

            step(i)

    def down(p, chips, step):
        owners = 2 * len(chips)

        @pl.loop(0, NB)
        def _(n):
            slot = (n + NB * (p + 1)) % 2
            dn_load(n, slot).wait()
            for e in range(EL):
                res = dot(act[e, 0:owners * SLOT], dn[slot, e])
                for i in range(owners):
                    o[i, e * SLOT:(e + 1) * SLOT] = res[i * SLOT:(i + 1) * SLOT]

            @pl.when(jnp.logical_or(n + 2 < NB, p < 2))
            def _():
                dn_load((n + 2) % NB, slot).start()

            for i in sorted(range(owners), key=lambda i: -(i % 2)):
                q = chips[i // 2]
                oo = o[i].astype(BF16)
                part = dot(comb[4 + i if q == DG else i], jnp.concatenate([oo, oo, oo], axis=0))
                if i % 2:
                    if p:
                        sibc(XN if p == 1 else YN, n).wait_send()
                    ss[SS_SLOT[q], n] = part
                    sibc(q, n).start()
                elif q == OWN:
                    acc[n] = acc[n] + part
                else:
                    s[q - 1, n] = part

            @pl.when(n > 0)
            def _():
                for q in chips:
                    finish(q, n - 1)

            step(n)

        for q in chips:
            finish(q, NB - 1)

    nothing = lambda i: None

    @pl.loop(0, 6)
    def _(i):
        build_comb(1 + i // 2, i % 2, i)

    for k, then in ((1, (7, 5)), (2, (8, 6)), (3, (9,)), (4, (10,))):
        agc(k).wait_recv()
        for c in then:
            agc(c).start()
    for k in (7, 8, 9, 10):
        agc(k).wait_recv()

    @pl.loop(0, 4)
    def _(i):
        dispatch(1 + i // 2, i % 2, i)

    gate_up(0, [XN, YN], nothing)
    for k, then in ((5, 11), (6, 12)):
        agc(k).wait_recv()
        agc(then).start()
    down(0, [XN, YN], nothing)

    agc(11).wait_recv()
    agc(12).wait_recv()
    for r in range(2):
        dispatch(DG, r, r)
    gate_up(1, [DG], nothing)
    down(1, [DG], nothing)

    def relay_gu(i):
        @pl.when(i % 3 == 1)
        def _():
            relay(i // 3)

    def relay_dn(n):
        @pl.when(n == 1)
        def _():
            relay(3)

        @pl.when(n == 4)
        def _():
            relay(4)

    agc(0).wait_recv()
    for r in range(2):
        build_comb(OWN, r, r)
        dispatch(OWN, r, r)
    gate_up(2, [OWN], relay_gu)
    down(2, [OWN], relay_dn)

    for n in range(NB):
        for k in (0, 5, 1, 4):
            icic(k, n).wait_recv()
        fin[:, n * BW:(n + 1) * BW] = (acc[n] + rx[n] + ry[n]).astype(BF16)
        out_copy(n).start()
    for n in range(NB):
        out_copy(n).wait()

    for k in range(NAG + len(PEERS)):
        agc(k).wait_send()
    for n in range(NB):
        for q in (DG, OWN):
            sibc(q, n).wait_send()
        for k in range(6):
            icic(k, n).wait_send()


def solution(mesh):
    def local_step(hidden, norm_gain, router_w, topk_idx, w_gate, w_up, w_down, shared_gate, shared_up, shared_down):
        T, H = hidden.shape
        EL, _, FF = w_gate.shape
        BW = 256
        NB = H // BW
        SLOT = 40
        NS = 4
        cfg = (T, H, FF, EL, SLOT, NB, BW, NS)
        vm = pl.BlockSpec(memory_space=pltpu.VMEM)
        anym = pl.BlockSpec(memory_space=pl.ANY)
        dma = pltpu.SemaphoreType.DMA
        n_ag = NAG + len(PEERS)
        return pl.pallas_call(
            functools.partial(moe_kernel, cfg),
            out_shape=jax.ShapeDtypeStruct((T, H), BF16),
            in_specs=[vm, vm, vm, vm] + [anym] * 6,
            out_specs=anym,
            scratch_shapes=[
                pltpu.VMEM((NS, H, 2 * FF), BF16),
                pltpu.VMEM((2, EL, FF, BW), BF16),
                pltpu.VMEM((4, 2, T, H), BF16),
                pltpu.VMEM((8, EL, T), F32),
                pltpu.VMEM((4, 2, EL, T), F32),
                pltpu.VMEM((4, 2, EL, T), F32),
                pltpu.VMEM((EL, 4 * SLOT, H), F32),
                pltpu.VMEM((EL, 4 * SLOT, FF), BF16),
                pltpu.VMEM((4, EL * SLOT, BW), F32),
                pltpu.VMEM((6, T, 3 * EL * SLOT), BF16),
                pltpu.VMEM((T, 2 * FF), BF16),
                pltpu.VMEM((NB, T, BW), F32),
                pltpu.VMEM((2, NB, T, BW), F32),
                pltpu.VMEM((3, NB, T, BW), F32),
                pltpu.VMEM((3, NB, T, BW), F32),
                pltpu.VMEM((NB, T, BW), F32),
                pltpu.VMEM((NB, T, BW), F32),
                pltpu.VMEM((NB, T // 2, BW), F32),
                pltpu.VMEM((NB, T // 2, BW), F32),
                pltpu.VMEM((T, H), BF16),
                dma((NS, 2)), dma((2,)), dma((NB,)),
                dma((n_ag,)), dma((n_ag,)), dma((4, NB)), dma((4, NB)), dma((6, NB)), dma((6, NB)),
            ],
            compiler_params=pltpu.CompilerParams(collective_id=0, has_side_effects=True, vmem_limit_bytes=67043328),
            name="moe_block",
        )(hidden, norm_gain, router_w.T, topk_idx.T, w_gate, w_up, w_down, shared_gate, shared_up,
          shared_down.reshape(2, FF, H))

    token_spec = P(('dp', 'ep'), None)
    expert_spec = P('ep', None, None)
    return jax.shard_map(
        local_step,
        mesh=mesh,
        in_specs=(token_spec, P(None), P(None, None), token_spec, expert_spec, expert_spec, expert_spec,
                  P(None, None), P(None, None), P(None, None)),
        out_specs=token_spec,
        check_vma=False,
    )
```

```python
import functools

import jax
import jax.numpy as jnp
from jax import lax
from jax.experimental import pallas as pl
from jax.experimental.pallas import tpu as pltpu
from jax.sharding import PartitionSpec as P

NORM_EPS = 1e-6
MESH = pl.DeviceIdType.MESH
F32 = jnp.float32
BF16 = jnp.bfloat16

OWN, XN, YN, DG = 0, 1, 2, 3
SR_SLOT = {XN: 0, YN: 1, DG: 2, OWN: 2}
SS_SLOT = {XN: 0, YN: 1, DG: 0, OWN: 1}
NAG = 13
PEERS = [(q, r) for q in range(4) for r in range(2) if (q, r) != (0, 0)]


def dot(a, b):
    return jnp.dot(a, b, preferred_element_type=F32)


def moe_kernel(cfg, hid, gain, rwt, topkt, wg, wu, wd, sg, su, sd, out,
               gu, dn, g, wloc, win, rankm, x, act, comb, ash, acc, ss, sr, s, rx, ry, qx, qy, fin, oall,
               gu_sem, dn_sem, out_sem, ag_s, ag_r, sib_s, sib_r, sbh_s, sbh_r, ici_s, ici_r):
    T, H, FF, EL, SLOT, NB, BW, NS = cfg
    HT = T // 2
    me = lax.axis_index("ep")
    core, xx, yy = me % 2, (me // 2) % 2, me // 4

    def ep_of(q, r):
        return 4 * ((yy + q // 2) % 2) + 2 * ((xx + q % 2) % 2) + (core + r) % 2

    def rcopy(src, dst, send, recv, q, r):
        return pltpu.make_async_remote_copy(src_ref=src, dst_ref=dst, send_sem=send, recv_sem=recv,
                                            device_id={"ep": ep_of(q, r)}, device_id_type=MESH)

    lo, hi = pl.ds(0, HT), pl.ds(HT, HT)
    ag = {
        0: (g.at[OWN, 0], g.at[OWN, 1], OWN, 1),
        1: (g.at[OWN, 0, lo], g.at[XN, 0, lo], XN, 0),
        2: (g.at[OWN, 0, hi], g.at[YN, 0, hi], YN, 0),
        3: (g.at[OWN, 0, hi], g.at[XN, 0, hi], XN, 0),
        4: (g.at[OWN, 0, lo], g.at[YN, 0, lo], YN, 0),
        5: (g.at[XN, 0, lo], g.at[DG, 0, lo], YN, 0),
        6: (g.at[YN, 0, hi], g.at[DG, 0, hi], XN, 0),
        7: (g.at[XN, 0, lo], g.at[XN, 1, lo], OWN, 1),
        8: (g.at[YN, 0, hi], g.at[YN, 1, hi], OWN, 1),
        9: (g.at[XN, 0, hi], g.at[XN, 1, hi], OWN, 1),
        10: (g.at[YN, 0, lo], g.at[YN, 1, lo], OWN, 1),
        11: (g.at[DG, 0, lo], g.at[DG, 1, lo], OWN, 1),
        12: (g.at[DG, 0, hi], g.at[DG, 1, hi], OWN, 1),
    }
    for j, (q, r) in enumerate(PEERS):
        ag[NAG + j] = (wloc.at[ep_of(q, r)], win.at[q, r], q, r)

    def agc(k):
        src, dst, q, r = ag[k]
        return rcopy(src, dst, ag_s.at[k], ag_r.at[k], q, r)

    def sibc(q, n):
        return rcopy(ss.at[SS_SLOT[q], n], sr.at[SR_SLOT[q], n], sib_s.at[q, n], sib_r.at[q, n], OWN, 1)

    direct = {XN: lo, YN: hi}
    later = {XN: hi, YN: lo}

    def sibh(q, n, half, b):
        return rcopy(ss.at[q - 1, n, half], sr.at[q - 1, n, half], sbh_s.at[b, q - 1, n], sbh_r.at[b, q - 1, n], OWN, 1)

    def icic(k, n):
        src, dst, q = [
            (s.at[XN - 1, n, lo], rx.at[n, lo], XN),
            (s.at[YN - 1, n, hi], ry.at[n, hi], YN),
            (s.at[DG - 1, n, lo], qx.at[n], XN),
            (s.at[DG - 1, n, hi], qy.at[n], YN),
            (s.at[YN - 1, n, lo], ry.at[n, lo], YN),
            (s.at[XN - 1, n, hi], rx.at[n, hi], XN),
        ][k]
        return rcopy(src, dst, ici_s.at[k, n], ici_r.at[k, n], q, 0)

    def gu_loads(e, slot):
        return [pltpu.make_async_copy(wg.at[e], gu.at[slot, :, pl.ds(0, FF)], gu_sem.at[slot, 0]),
                pltpu.make_async_copy(wu.at[e], gu.at[slot, :, pl.ds(FF, FF)], gu_sem.at[slot, 1])]

    def dn_load(n, slot):
        return pltpu.make_async_copy(wd.at[:, :, pl.ds(pl.multiple_of(n * BW, BW), BW)], dn.at[slot], dn_sem.at[slot])

    def sd_load(n, slot):
        return pltpu.make_async_copy(sd.at[:, :, pl.ds(pl.multiple_of(n * BW, BW), BW)], dn.at[slot, pl.ds(0, 2)],
                                     dn_sem.at[slot])

    def out_copy(n):
        cols = pl.ds(n * BW, BW)
        return pltpu.make_async_copy(fin.at[:, cols], out.at[:, cols], out_sem.at[n])

    sg_load = pltpu.make_async_copy(sg, gu.at[NS - 2], gu_sem.at[NS - 2, 0])
    su_load = pltpu.make_async_copy(su, gu.at[NS - 1], gu_sem.at[NS - 1, 0])
    sg_load.start()
    su_load.start()
    sd_load(0, 0).start()
    sd_load(1, 1).start()

    barrier = pltpu.get_barrier_semaphore()
    for q, r in PEERS:
        pl.semaphore_signal(barrier, inc=1, device_id={"ep": ep_of(q, r)}, device_id_type=MESH)

    h = hid[...].astype(F32)
    inv = lax.rsqrt(jnp.mean(h * h, axis=-1, keepdims=True) + NORM_EPS)
    g[OWN, 0] = (h * inv * gain[...][None, :]).astype(BF16)

    logits = lax.dot_general(rwt[...], g[OWN, 0], (((1,), (1,)), ((), ())), preferred_element_type=F32)
    ex = jnp.exp(logits - jnp.max(logits, axis=0, keepdims=True))
    p = ex / jnp.sum(ex, axis=0, keepdims=True)
    expert = lax.broadcasted_iota(jnp.int32, logits.shape, 0)
    chosen = topkt[0:1, :] == expert
    for j in range(1, topkt.shape[0]):
        chosen = jnp.logical_or(chosen, topkt[j:j + 1, :] == expert)
    wloc[...] = jnp.where(chosen, p, -1.0).reshape(8, EL, T)
    pl.semaphore_wait(barrier, len(PEERS))
    agc(1).start()
    agc(2).start()
    for j in range(len(PEERS)):
        agc(NAG + j).start()
    for k in (0, 3, 4):
        agc(k).start()
    win[OWN, 0] = wloc[me]

    sg_load.wait()
    su_load.wait()
    for e in range(NS - 2):
        for c in gu_loads(e, e):
            c.start()

    @pl.loop(0, ash.shape[1] // BW)
    def _(n):
        cols = pl.ds(pl.multiple_of(n * BW, BW), BW)
        ga = dot(g[OWN, 0], gu[NS - 2, :, cols])
        up = dot(g[OWN, 0], gu[NS - 1, :, cols])
        ash[:, cols] = (jax.nn.silu(ga) * up).astype(BF16)

    for e in (NS - 2, NS - 1):
        for c in gu_loads(e, e):
            c.start()

    @pl.loop(0, NB)
    def _(n):
        cols = pl.ds(pl.multiple_of(n * BW, BW), BW)
        slot = n % 2
        sd_load(n, slot).wait()
        acc[n] = hid[:, cols].astype(F32) + dot(ash[...], dn[slot, 0:2].reshape(2 * FF, BW))

        @pl.when(n + 2 < NB)
        def _():
            sd_load(n + 2, slot).start()

        @pl.when(n + 2 >= NB)
        def _():
            dn_load(n + 2 - NB, slot).start()

    for j in range(len(PEERS)):
        agc(NAG + j).wait_recv()
    wall = win[...].reshape(8 * EL, T)
    upper = (lax.broadcasted_iota(jnp.int32, (T, T), 0) < lax.broadcasted_iota(jnp.int32, (T, T), 1))
    upper = jnp.where(upper, 1.0, 0.0).astype(BF16)
    rank = dot(jnp.where(wall >= 0, 1.0, 0.0).astype(BF16), upper)
    rankm[...] = jnp.where(wall >= 0, rank, -1.0).reshape(4, 2, EL, T)

    def hits(q, r):
        slot_id = lax.broadcasted_iota(jnp.int32, (EL, SLOT, T), 1).astype(F32)
        return jnp.broadcast_to(rankm[q, r][:, None, :], (EL, SLOT, T)) == slot_id

    def dispatch(q, r, i):
        pick = jnp.where(hits(q, r), 1.0, 0.0).reshape(EL * SLOT, T).astype(BF16)
        x[:, pl.ds(pl.multiple_of(i * SLOT, SLOT), SLOT)] = dot(pick, g[q, r]).reshape(EL, SLOT, H)

    def build_comb(q, r, i):
        w = jnp.broadcast_to(win[q, r][:, None, :], (EL, SLOT, T))
        cw = jnp.where(hits(q, r), w, 0.0).reshape(EL * SLOT, T)
        c1 = cw.astype(BF16).astype(F32)
        c2 = (cw - c1).astype(BF16).astype(F32)
        comb[i] = jnp.concatenate([c1, c2, cw - c1 - c2], axis=0).T.astype(BF16)

    def finish(q, n):
        if q in direct:
            half = direct[q]
            sibh(q, n, half, 0).wait_recv()
            s[q - 1, n, half] = s[q - 1, n, half] + sr[q - 1, n, half]
            icic(q - 1, n).start()
            return
        sibc(q, n).wait_recv()
        if q == OWN:
            acc[n] = acc[n] + sr[SR_SLOT[q], n]
            return
        s[q - 1, n] = s[q - 1, n] + sr[SR_SLOT[q], n]
        icic(2, n).start()
        icic(3, n).start()

    def deferred(n):
        sibc(DG, n).wait_send()
        for q in (XN, YN):
            i = 2 * (q - 1) + 1
            oo = oall[n, i]
            ss[q - 1, n, later[q]] = dot(comb[i, later[q]], jnp.concatenate([oo, oo, oo], axis=0))
            sibh(q, n, later[q], 1).start()
        for q in (XN, YN):
            i = 2 * (q - 1)
            oo = oall[n, i]
            s[q - 1, n, later[q]] = dot(comb[i, later[q]], jnp.concatenate([oo, oo, oo], axis=0))

    def relay(n):
        for q, k, buf in ((YN, 2, qx), (XN, 3, qy)):
            sibh(q, n, later[q], 1).wait_recv()
            icic(k, n).wait_recv()
            s[q - 1, n, later[q]] = s[q - 1, n, later[q]] + sr[q - 1, n, later[q]] + buf[n]
            icic(k + 2, n).start()

    def gate_up(p, chips, step):
        rows = 2 * len(chips) * SLOT

        @pl.loop(0, EL)
        def _(i):
            e = EL - 1 - i if p % 2 else i
            slot = e % NS

            @pl.when(i >= (NS if p else 0))
            def _():
                for c in gu_loads(e, slot):
                    c.wait()

            gua = dot(x[e, 0:rows].astype(BF16), gu[slot])
            act[e, 0:rows] = (jax.nn.silu(gua[:, 0:FF]) * gua[:, FF:2 * FF]).astype(BF16)

            @pl.when(i < EL - NS)
            def _():
                for c in gu_loads(e - NS if p % 2 else e + NS, slot):
                    c.start()

            step(i)

    def down(p, chips, step):
        owners = 2 * len(chips)

        @pl.loop(0, NB)
        def _(n):
            slot = (n + NB * (p + 1)) % 2
            dn_load(n, slot).wait()
            for e in range(EL):
                res = dot(act[e, 0:owners * SLOT], dn[slot, e])
                for i in range(owners):
                    x[i, e % 4 * SLOT:(e % 4 + 1) * SLOT, e // 4 * BW:(e // 4 + 1) * BW] = res[i * SLOT:(i + 1) * SLOT]

            @pl.when(jnp.logical_or(n + 2 < NB, p < 2))
            def _():
                dn_load((n + 2) % NB, slot).start()

            for i in sorted(range(owners), key=lambda i: -(i % 2)):
                q = chips[i // 2]
                if i == owners - 2 - 2 * (owners == 4):
                    @pl.when(n == 1)
                    def _():
                        for c in chips:
                            finish(c, 0)

                oo = jnp.concatenate([x[i, :, 0:BW], x[i, :, BW:2 * BW]], axis=0).astype(BF16)
                stack = jnp.concatenate([oo, oo, oo], axis=0)
                if q in direct:
                    half = direct[q]
                    oall[n, i] = oo
                    part = dot(comb[i, half], stack)
                    if i % 2:
                        ss[q - 1, n, half] = part
                        sibh(q, n, half, 0).start()
                    else:
                        s[q - 1, n, half] = part
                    continue
                part = dot(comb[4 + i], stack)
                if i % 2:
                    if q == DG:
                        sibh(XN, n, direct[XN], 0).wait_send()
                    else:
                        sibh(YN, n, direct[YN], 0).wait_send()
                        sibh(YN, n, later[YN], 1).wait_send()
                    ss[SS_SLOT[q], n] = part
                    sibc(q, n).start()
                elif q == OWN:
                    acc[n] = acc[n] + part
                else:
                    s[q - 1, n] = part

            @pl.when(n > 1)
            def _():
                for q in chips:
                    finish(q, n - 1)

            step(n)

        for q in chips:
            finish(q, NB - 1)

    nothing = lambda i: None

    @pl.loop(0, 6)
    def _(i):
        build_comb(1 + i // 2, i % 2, i)

    for k, then in ((1, (7, 5)), (2, (8, 6)), (3, (9,)), (4, (10,))):
        agc(k).wait_recv()
        for c in then:
            agc(c).start()
    dispatch(XN, 0, 0)
    dispatch(YN, 0, 2)
    for k in (7, 8, 9, 10):
        agc(k).wait_recv()
    dispatch(XN, 1, 1)
    dispatch(YN, 1, 3)

    gate_up(0, [XN, YN], nothing)
    for k, then in ((5, 11), (6, 12)):
        agc(k).wait_recv()
        agc(then).start()
    down(0, [XN, YN], nothing)

    agc(11).wait_recv()
    agc(12).wait_recv()
    for r in range(2):
        dispatch(DG, r, r)
    gate_up(1, [DG], nothing)
    down(1, [DG], nothing)

    def relay_gu(i):
        @pl.when(i % 2 == 1)
        def _():
            relay(i // 2)

    def relay_dn(n):
        @pl.when(n == 1)
        def _():
            relay(4)

    @pl.loop(0, NB)
    def _(n):
        deferred(n)

    agc(0).wait_recv()
    for r in range(2):
        build_comb(OWN, r, 4 + r)
        dispatch(OWN, r, r)
    gate_up(2, [OWN], relay_gu)
    down(2, [OWN], relay_dn)

    for n in range(NB):
        for k in (0, 5, 1, 4):
            icic(k, n).wait_recv()
        fin[:, n * BW:(n + 1) * BW] = (acc[n] + rx[n] + ry[n]).astype(BF16)
        out_copy(n).start()
    for n in range(NB):
        out_copy(n).wait()

    for k in range(NAG + len(PEERS)):
        agc(k).wait_send()
    for n in range(NB):
        sibc(OWN, n).wait_send()
        sibh(XN, n, later[XN], 1).wait_send()
        for k in range(6):
            icic(k, n).wait_send()


def solution(mesh):
    def local_step(hidden, norm_gain, router_w, topk_idx, w_gate, w_up, w_down, shared_gate, shared_up, shared_down):
        T, H = hidden.shape
        EL, _, FF = w_gate.shape
        BW = 256
        NB = H // BW
        SLOT = 40
        NS = 4
        cfg = (T, H, FF, EL, SLOT, NB, BW, NS)
        vm = pl.BlockSpec(memory_space=pltpu.VMEM)
        anym = pl.BlockSpec(memory_space=pl.ANY)
        dma = pltpu.SemaphoreType.DMA
        n_ag = NAG + len(PEERS)
        return pl.pallas_call(
            functools.partial(moe_kernel, cfg),
            out_shape=jax.ShapeDtypeStruct((T, H), BF16),
            in_specs=[vm, vm, vm, vm] + [anym] * 6,
            out_specs=anym,
            scratch_shapes=[
                pltpu.VMEM((NS, H, 2 * FF), BF16),
                pltpu.VMEM((2, EL, FF, BW), BF16),
                pltpu.VMEM((4, 2, T, H), BF16),
                pltpu.VMEM((8, EL, T), F32),
                pltpu.VMEM((4, 2, EL, T), F32),
                pltpu.VMEM((4, 2, EL, T), F32),
                pltpu.VMEM((EL, 4 * SLOT, H), F32),
                pltpu.VMEM((EL, 4 * SLOT, FF), BF16),
                pltpu.VMEM((6, T, 3 * EL * SLOT), BF16),
                pltpu.VMEM((T, 2 * FF), BF16),
                pltpu.VMEM((NB, T, BW), F32),
                pltpu.VMEM((2, NB, T, BW), F32),
                pltpu.VMEM((3, NB, T, BW), F32),
                pltpu.VMEM((3, NB, T, BW), F32),
                pltpu.VMEM((NB, T, BW), F32),
                pltpu.VMEM((NB, T, BW), F32),
                pltpu.VMEM((NB, T // 2, BW), F32),
                pltpu.VMEM((NB, T // 2, BW), F32),
                pltpu.VMEM((T, H), BF16),
                pltpu.VMEM((NB, 4, EL * SLOT, BW), BF16),
                dma((NS, 2)), dma((2,)), dma((NB,)),
                dma((n_ag,)), dma((n_ag,)), dma((4, NB)), dma((4, NB)), dma((2, 2, NB)), dma((2, 2, NB)), dma((6, NB)), dma((6, NB)),
            ],
            compiler_params=pltpu.CompilerParams(collective_id=0, has_side_effects=True, vmem_limit_bytes=67043328),
            name="moe_block",
        )(hidden, norm_gain, router_w.T, topk_idx.T, w_gate, w_up, w_down, shared_gate, shared_up,
          shared_down.reshape(2, FF, H))

    token_spec = P(('dp', 'ep'), None)
    expert_spec = P('ep', None, None)
    return jax.shard_map(
        local_step,
        mesh=mesh,
        in_specs=(token_spec, P(None), P(None, None), token_spec, expert_spec, expert_spec, expert_spec,
                  P(None, None), P(None, None), P(None, None)),
        out_specs=token_spec,
        check_vma=False,
    )
```

```python
import functools

import jax
import jax.numpy as jnp
from jax import lax
from jax.experimental import pallas as pl
from jax.experimental.pallas import tpu as pltpu
from jax.sharding import PartitionSpec as P

NORM_EPS = 1e-6
MESH = pl.DeviceIdType.MESH
F32 = jnp.float32
BF16 = jnp.bfloat16

OWN, XN, YN, DG = 0, 1, 2, 3
SR_SLOT = {XN: 0, YN: 1, DG: 2, OWN: 2}
SS_SLOT = {XN: 0, YN: 1, DG: 0, OWN: 1}
NAG = 13
PEERS = [(q, r) for q in range(4) for r in range(2) if (q, r) != (0, 0)]


def dot(a, b):
    return jnp.dot(a, b, preferred_element_type=F32)


def moe_kernel(cfg, hid, gain, rwt, topkt, wg, wu, wd, sg, su, sd, out,
               gu, dn, g, wloc, win, rankm, x, act, comb, ash, acc, ss, sr, s, rx, ry, qx, qy, fin, oall,
               gu_sem, dn_sem, out_sem, ag_s, ag_r, sib_s, sib_r, sbh_s, sbh_r, ici_s, ici_r):
    T, H, FF, EL, SLOT, NB, BW, NS = cfg
    HT = T // 2
    me = lax.axis_index("ep")
    core, xx, yy = me % 2, (me // 2) % 2, me // 4

    def ep_of(q, r):
        return 4 * ((yy + q // 2) % 2) + 2 * ((xx + q % 2) % 2) + (core + r) % 2

    def rcopy(src, dst, send, recv, q, r):
        return pltpu.make_async_remote_copy(src_ref=src, dst_ref=dst, send_sem=send, recv_sem=recv,
                                            device_id={"ep": ep_of(q, r)}, device_id_type=MESH)

    lo, hi = pl.ds(0, HT), pl.ds(HT, HT)
    ag = {
        0: (g.at[OWN, 0], g.at[OWN, 1], OWN, 1),
        1: (g.at[OWN, 0, lo], g.at[XN, 0, lo], XN, 0),
        2: (g.at[OWN, 0, hi], g.at[YN, 0, hi], YN, 0),
        3: (g.at[OWN, 0, hi], g.at[XN, 0, hi], XN, 0),
        4: (g.at[OWN, 0, lo], g.at[YN, 0, lo], YN, 0),
        5: (g.at[XN, 0, lo], g.at[DG, 0, lo], YN, 0),
        6: (g.at[YN, 0, hi], g.at[DG, 0, hi], XN, 0),
        7: (g.at[XN, 0, lo], g.at[XN, 1, lo], OWN, 1),
        8: (g.at[YN, 0, hi], g.at[YN, 1, hi], OWN, 1),
        9: (g.at[XN, 0, hi], g.at[XN, 1, hi], OWN, 1),
        10: (g.at[YN, 0, lo], g.at[YN, 1, lo], OWN, 1),
        11: (g.at[DG, 0, lo], g.at[DG, 1, lo], OWN, 1),
        12: (g.at[DG, 0, hi], g.at[DG, 1, hi], OWN, 1),
    }
    for j, (q, r) in enumerate(PEERS):
        ag[NAG + j] = (wloc.at[ep_of(q, r)], win.at[q, r], q, r)

    def agc(k):
        src, dst, q, r = ag[k]
        return rcopy(src, dst, ag_s.at[k], ag_r.at[k], q, r)

    def sibc(q, n):
        return rcopy(ss.at[SS_SLOT[q], n], sr.at[SR_SLOT[q], n], sib_s.at[q, n], sib_r.at[q, n], OWN, 1)

    direct = {XN: lo, YN: hi}
    later = {XN: hi, YN: lo}

    def sibh(q, n, half, b):
        return rcopy(ss.at[q - 1, n, half], sr.at[q - 1, n, half], sbh_s.at[b, q - 1, n], sbh_r.at[b, q - 1, n], OWN, 1)

    def icic(k, n):
        src, dst, q = [
            (s.at[XN - 1, n, lo], rx.at[n, lo], XN),
            (s.at[YN - 1, n, hi], ry.at[n, hi], YN),
            (s.at[DG - 1, n, lo], qx.at[n], XN),
            (s.at[DG - 1, n, hi], qy.at[n], YN),
            (s.at[YN - 1, n, lo], ry.at[n, lo], YN),
            (s.at[XN - 1, n, hi], rx.at[n, hi], XN),
        ][k]
        return rcopy(src, dst, ici_s.at[k, n], ici_r.at[k, n], q, 0)

    def gu_loads(e, slot):
        return [pltpu.make_async_copy(wg.at[e], gu.at[slot, :, pl.ds(0, FF)], gu_sem.at[slot, 0]),
                pltpu.make_async_copy(wu.at[e], gu.at[slot, :, pl.ds(FF, FF)], gu_sem.at[slot, 1])]

    def dn_load(n, slot):
        return pltpu.make_async_copy(wd.at[:, :, pl.ds(pl.multiple_of(n * BW, BW), BW)], dn.at[slot], dn_sem.at[slot])

    def sd_load(n, slot):
        return pltpu.make_async_copy(sd.at[:, :, pl.ds(pl.multiple_of(n * BW, BW), BW)], dn.at[slot, pl.ds(0, 2)],
                                     dn_sem.at[slot])

    def out_copy(n):
        cols = pl.ds(n * BW, BW)
        return pltpu.make_async_copy(fin.at[:, cols], out.at[:, cols], out_sem.at[n])

    sg_load = pltpu.make_async_copy(sg, gu.at[NS - 2], gu_sem.at[NS - 2, 0])
    su_load = pltpu.make_async_copy(su, gu.at[NS - 1], gu_sem.at[NS - 1, 0])
    sg_load.start()
    su_load.start()
    sd_load(0, 0).start()
    sd_load(1, 1).start()

    barrier = pltpu.get_barrier_semaphore()
    for q, r in PEERS:
        pl.semaphore_signal(barrier, inc=1, device_id={"ep": ep_of(q, r)}, device_id_type=MESH)

    h = hid[...].astype(F32)
    inv = lax.rsqrt(jnp.mean(h * h, axis=-1, keepdims=True) + NORM_EPS)
    g[OWN, 0] = (h * inv * gain[...][None, :]).astype(BF16)

    logits = lax.dot_general(rwt[...], g[OWN, 0], (((1,), (1,)), ((), ())), preferred_element_type=F32)
    ex = jnp.exp(logits - jnp.max(logits, axis=0, keepdims=True))
    p = ex / jnp.sum(ex, axis=0, keepdims=True)
    expert = lax.broadcasted_iota(jnp.int32, logits.shape, 0)
    chosen = topkt[0:1, :] == expert
    for j in range(1, topkt.shape[0]):
        chosen = jnp.logical_or(chosen, topkt[j:j + 1, :] == expert)
    wloc[...] = jnp.where(chosen, p, -1.0).reshape(8, EL, T)
    pl.semaphore_wait(barrier, len(PEERS))
    agc(1).start()
    agc(2).start()
    for j in range(len(PEERS)):
        agc(NAG + j).start()
    for k in (0, 3, 4):
        agc(k).start()
    win[OWN, 0] = wloc[me]

    sg_load.wait()
    su_load.wait()
    for e in range(NS - 2):
        for c in gu_loads(e, e):
            c.start()

    @pl.loop(0, ash.shape[1] // BW)
    def _(n):
        cols = pl.ds(pl.multiple_of(n * BW, BW), BW)
        ga = dot(g[OWN, 0], gu[NS - 2, :, cols])
        up = dot(g[OWN, 0], gu[NS - 1, :, cols])
        ash[:, cols] = (jax.nn.silu(ga) * up).astype(BF16)

    for e in (NS - 2, NS - 1):
        for c in gu_loads(e, e):
            c.start()

    @pl.loop(0, NB)
    def _(n):
        cols = pl.ds(pl.multiple_of(n * BW, BW), BW)
        slot = n % 2
        sd_load(n, slot).wait()
        acc[n] = hid[:, cols].astype(F32) + dot(ash[...], dn[slot, 0:2].reshape(2 * FF, BW))

        @pl.when(n + 2 < NB)
        def _():
            sd_load(n + 2, slot).start()

        @pl.when(n + 2 >= NB)
        def _():
            dn_load(n + 2 - NB, slot).start()

    for j in range(len(PEERS)):
        agc(NAG + j).wait_recv()
    wall = win[...].reshape(8 * EL, T)
    upper = (lax.broadcasted_iota(jnp.int32, (T, T), 0) < lax.broadcasted_iota(jnp.int32, (T, T), 1))
    upper = jnp.where(upper, 1.0, 0.0).astype(BF16)
    rank = dot(jnp.where(wall >= 0, 1.0, 0.0).astype(BF16), upper)
    rankm[...] = jnp.where(wall >= 0, rank, -1.0).reshape(4, 2, EL, T)

    def hits(q, r):
        slot_id = lax.broadcasted_iota(jnp.int32, (EL, SLOT, T), 1).astype(F32)
        return jnp.broadcast_to(rankm[q, r][:, None, :], (EL, SLOT, T)) == slot_id

    def dispatch(q, r, i):
        pick = jnp.where(hits(q, r), 1.0, 0.0).reshape(EL * SLOT, T).astype(BF16)
        x[:, pl.ds(pl.multiple_of(i * SLOT, SLOT), SLOT)] = dot(pick, g[q, r]).reshape(EL, SLOT, H)

    def build_comb(q, r, i):
        w = jnp.broadcast_to(win[q, r][:, None, :], (EL, SLOT, T))
        cw = jnp.where(hits(q, r), w, 0.0).reshape(EL * SLOT, T)
        c1 = cw.astype(BF16).astype(F32)
        c2 = (cw - c1).astype(BF16).astype(F32)
        comb[i] = jnp.concatenate([c1, c2, cw - c1 - c2], axis=0).T.astype(BF16)

    def finish(q, n):
        if q in direct:
            half = direct[q]
            sibh(q, n, half, 0).wait_recv()
            s[q - 1, n, half] = s[q - 1, n, half] + sr[q - 1, n, half]
            icic(q - 1, n).start()
            return
        sibc(q, n).wait_recv()
        if q == OWN:
            acc[n] = acc[n] + sr[SR_SLOT[q], n]
            return
        s[q - 1, n] = s[q - 1, n] + sr[SR_SLOT[q], n]
        icic(2, n).start()
        icic(3, n).start()

    def deferred(n):
        sibc(DG, n).wait_send()
        for q in (XN, YN):
            i = 2 * (q - 1) + 1
            oo = oall[n, i]
            ss[q - 1, n, later[q]] = dot(comb[i, later[q]], jnp.concatenate([oo, oo, oo], axis=0))
            sibh(q, n, later[q], 1).start()
        for q in (XN, YN):
            i = 2 * (q - 1)
            oo = oall[n, i]
            s[q - 1, n, later[q]] = dot(comb[i, later[q]], jnp.concatenate([oo, oo, oo], axis=0))

    def relay(n):
        for q, k, buf in ((YN, 2, qx), (XN, 3, qy)):
            sibh(q, n, later[q], 1).wait_recv()
            icic(k, n).wait_recv()
            s[q - 1, n, later[q]] = s[q - 1, n, later[q]] + sr[q - 1, n, later[q]] + buf[n]
            icic(k + 2, n).start()

    def gate_up(p, chips, step):
        rows = 2 * len(chips) * SLOT

        @pl.loop(0, EL)
        def _(i):
            e = EL - 1 - i if p % 2 else i
            slot = e % NS

            @pl.when(i >= (NS if p else 0))
            def _():
                for c in gu_loads(e, slot):
                    c.wait()

            gua = dot(x[e, 0:rows].astype(BF16), gu[slot])
            act[e, 0:rows] = (jax.nn.silu(gua[:, 0:FF]) * gua[:, FF:2 * FF]).astype(BF16)

            @pl.when(i < EL - NS)
            def _():
                for c in gu_loads(e - NS if p % 2 else e + NS, slot):
                    c.start()

            step(i)

    def down(p, chips, step):
        owners = 2 * len(chips)

        @pl.loop(0, NB)
        def _(n):
            slot = (n + NB * (p + 1)) % 2
            dn_load(n, slot).wait()
            for e in range(EL):
                res = dot(act[e, 0:owners * SLOT], dn[slot, e])
                for i in range(owners):
                    x[i, e % 4 * SLOT:(e % 4 + 1) * SLOT, e // 4 * BW:(e // 4 + 1) * BW] = res[i * SLOT:(i + 1) * SLOT]

            @pl.when(jnp.logical_or(n + 2 < NB, p < 2))
            def _():
                dn_load((n + 2) % NB, slot).start()

            for i in sorted(range(owners), key=lambda i: -(i % 2)):
                q = chips[i // 2]
                if i == owners - 2 - 2 * (owners == 4):
                    @pl.when(n == 1)
                    def _():
                        for c in chips:
                            finish(c, 0)

                oo = jnp.concatenate([x[i, :, 0:BW], x[i, :, BW:2 * BW]], axis=0).astype(BF16)
                stack = jnp.concatenate([oo, oo, oo], axis=0)
                if q in direct:
                    half = direct[q]
                    oall[n, i] = oo
                    part = dot(comb[i, half], stack)
                    if i % 2:
                        ss[q - 1, n, half] = part
                        sibh(q, n, half, 0).start()
                    else:
                        s[q - 1, n, half] = part
                    continue
                part = dot(comb[4 + i], stack)
                if i % 2:
                    if q == DG:
                        sibh(XN, n, direct[XN], 0).wait_send()
                    else:
                        sibh(YN, n, direct[YN], 0).wait_send()
                        sibh(YN, n, later[YN], 1).wait_send()
                    ss[SS_SLOT[q], n] = part
                    sibc(q, n).start()
                elif q == OWN:
                    acc[n] = acc[n] + part
                else:
                    s[q - 1, n] = part

            @pl.when(n > 1)
            def _():
                for q in chips:
                    finish(q, n - 1)

            step(n)

        for q in chips:
            finish(q, NB - 1)

    nothing = lambda i: None

    @pl.loop(0, 6)
    def _(i):
        build_comb(1 + i // 2, i % 2, i)

    for k, then in ((1, (7,)), (2, (8,)), (3, (9,)), (4, (10, 5, 6))):
        agc(k).wait_recv()
        for c in then:
            agc(c).start()
    dispatch(XN, 0, 0)
    dispatch(YN, 0, 2)
    for k in (7, 8, 9, 10):
        agc(k).wait_recv()
    dispatch(XN, 1, 1)
    dispatch(YN, 1, 3)

    gate_up(0, [XN, YN], nothing)
    for k, then in ((5, 11), (6, 12)):
        agc(k).wait_recv()
        agc(then).start()
    down(0, [XN, YN], nothing)

    agc(11).wait_recv()
    agc(12).wait_recv()
    for r in range(2):
        dispatch(DG, r, r)
    gate_up(1, [DG], nothing)
    down(1, [DG], nothing)

    def relay_gu(i):
        @pl.when(i % 2 == 1)
        def _():
            relay(i // 2)

    def relay_dn(n):
        @pl.when(n == 1)
        def _():
            relay(4)

    @pl.loop(0, NB)
    def _(n):
        deferred(n)

    agc(0).wait_recv()
    for r in range(2):
        build_comb(OWN, r, 4 + r)
        dispatch(OWN, r, r)
    gate_up(2, [OWN], relay_gu)
    down(2, [OWN], relay_dn)

    for n in range(NB):
        for k in (0, 5, 1, 4):
            icic(k, n).wait_recv()
        fin[:, n * BW:(n + 1) * BW] = (acc[n] + rx[n] + ry[n]).astype(BF16)
        out_copy(n).start()
    for n in range(NB):
        out_copy(n).wait()

    for k in range(NAG + len(PEERS)):
        agc(k).wait_send()
    for n in range(NB):
        sibc(OWN, n).wait_send()
        sibh(XN, n, later[XN], 1).wait_send()
        for k in range(6):
            icic(k, n).wait_send()


def solution(mesh):
    def local_step(hidden, norm_gain, router_w, topk_idx, w_gate, w_up, w_down, shared_gate, shared_up, shared_down):
        T, H = hidden.shape
        EL, _, FF = w_gate.shape
        BW = 256
        NB = H // BW
        SLOT = 40
        NS = 4
        cfg = (T, H, FF, EL, SLOT, NB, BW, NS)
        vm = pl.BlockSpec(memory_space=pltpu.VMEM)
        anym = pl.BlockSpec(memory_space=pl.ANY)
        dma = pltpu.SemaphoreType.DMA
        n_ag = NAG + len(PEERS)
        return pl.pallas_call(
            functools.partial(moe_kernel, cfg),
            out_shape=jax.ShapeDtypeStruct((T, H), BF16),
            in_specs=[vm, vm, vm, vm] + [anym] * 6,
            out_specs=anym,
            scratch_shapes=[
                pltpu.VMEM((NS, H, 2 * FF), BF16),
                pltpu.VMEM((2, EL, FF, BW), BF16),
                pltpu.VMEM((4, 2, T, H), BF16),
                pltpu.VMEM((8, EL, T), F32),
                pltpu.VMEM((4, 2, EL, T), F32),
                pltpu.VMEM((4, 2, EL, T), F32),
                pltpu.VMEM((EL, 4 * SLOT, H), F32),
                pltpu.VMEM((EL, 4 * SLOT, FF), BF16),
                pltpu.VMEM((6, T, 3 * EL * SLOT), BF16),
                pltpu.VMEM((T, 2 * FF), BF16),
                pltpu.VMEM((NB, T, BW), F32),
                pltpu.VMEM((2, NB, T, BW), F32),
                pltpu.VMEM((3, NB, T, BW), F32),
                pltpu.VMEM((3, NB, T, BW), F32),
                pltpu.VMEM((NB, T, BW), F32),
                pltpu.VMEM((NB, T, BW), F32),
                pltpu.VMEM((NB, T // 2, BW), F32),
                pltpu.VMEM((NB, T // 2, BW), F32),
                pltpu.VMEM((T, H), BF16),
                pltpu.VMEM((NB, 4, EL * SLOT, BW), BF16),
                dma((NS, 2)), dma((2,)), dma((NB,)),
                dma((n_ag,)), dma((n_ag,)), dma((4, NB)), dma((4, NB)), dma((2, 2, NB)), dma((2, 2, NB)), dma((6, NB)), dma((6, NB)),
            ],
            compiler_params=pltpu.CompilerParams(collective_id=0, has_side_effects=True, vmem_limit_bytes=67043328),
            name="moe_block",
        )(hidden, norm_gain, router_w.T, topk_idx.T, w_gate, w_up, w_down, shared_gate, shared_up,
          shared_down.reshape(2, FF, H))

    token_spec = P(('dp', 'ep'), None)
    expert_spec = P('ep', None, None)
    return jax.shard_map(
        local_step,
        mesh=mesh,
        in_specs=(token_spec, P(None), P(None, None), token_spec, expert_spec, expert_spec, expert_spec,
                  P(None, None), P(None, None), P(None, None)),
        out_specs=token_spec,
        check_vma=False,
    )
```
